32 devices in a mesh: dp: 4 (over x, core), expert: 8 (over z, y).
Axes of the slice: x: 2, y: 2, z: 4, core: 2. Of those that a mesh axis runs over, the one named last changes fastest.
Arguments:
- tokens: bfloat16 [128, 256, 1280], P(('dp', 'expert')), may hold values from -32 to 32
- slot_keys: bfloat16 [1280, 8], replicated, may hold values from -20 to 20
- logit_scale: float32 [1], replicated, may hold values from 8 to 16
- up_weight: bfloat16 [8, 1280, 5120], P('expert', None, 'dp'), may hold values from -0.15625 to 0.15625
- up_bias: bfloat16 [8, 5120], P('expert', 'dp'), may hold values from -3 to 3
- down_weight: bfloat16 [8, 5120, 1280], P('expert', 'dp'), may hold values from -0.078125 to 0.078125
- down_bias: bfloat16 [8, 1280], replicated, may hold values from -3 to 3
Outputs:
- mixed_out: bfloat16 [128, 256, 1280], P(('dp', 'expert'))
The draws below stay inside these ranges and needn't reach their ends.
All inputs are finite; a program needn't handle non-finite values.
Results may differ from the reference program's by a relative error of at most 0.017.
Values may be sent and summed in bfloat16 or wider, within the bound.
A program may use at most 64 MiB of HBM per device.

```python
import math
import jax
import jax.numpy as jnp
from jax import lax

D = 1280
FF = 5120
PATCHES = 256
EXPERTS = 8
IMAGES = 128
N_DP = 4


def slot_basis(key):
    raw = jax.random.normal(jax.random.fold_in(key, 11), (D, EXPERTS), jnp.float32)
    return jnp.clip(raw, -4.0, 4.0)


def draw_slot_keys(key, part):
    basis = slot_basis(key)
    column_scale = jnp.exp(jax.random.uniform(jax.random.fold_in(key, 12), (1, EXPERTS), jnp.float32, math.log(0.5), math.log(5.0)))
    return (basis * column_scale).astype(jnp.bfloat16)


def draw_tokens(key, part):
    basis = slot_basis(key)
    rows_total = IMAGES * PATCHES
    coeffs = jnp.clip(jax.random.normal(jax.random.fold_in(key, 13), (rows_total, EXPERTS), jnp.float32), -4.0, 4.0)
    mixture = 0.2 * jnp.dot(coeffs, jnp.transpose(basis))
    noise = jnp.clip(jax.random.normal(jax.random.fold_in(key, 14), (rows_total, D), jnp.float32), -4.0, 4.0)
    row_scale = jnp.exp(jax.random.uniform(jax.random.fold_in(key, 15), (rows_total, 1), jnp.float32, math.log(0.5), math.log(5.0)))
    values = jnp.clip(row_scale * (noise + mixture), -32.0, 32.0)
    return values.reshape(IMAGES, PATCHES, D).astype(jnp.bfloat16)


def level_of(own_key, shape, pieces, smallest, largest):
    factor_of = 1.0
    for dim, blocks in pieces:
        draws = jax.random.uniform(jax.random.fold_in(jax.random.fold_in(own_key, 6), dim), (blocks,), jnp.float32, smallest / len(pieces), largest / len(pieces))
        factor_of = factor_of * jnp.repeat(jnp.exp(draws), shape[dim] // blocks).reshape((-1,) + (1,) * (len(shape) - 1 - dim))
    return factor_of


def bell_draw(key, dims, scale, bound, cuts=(), held_as=jnp.bfloat16):
    entries = scale * jax.random.normal(key, dims, jnp.float32)
    if cuts:
        entries = entries * level_of(key, dims, cuts, -0.22, 0.18)
    return jnp.clip(entries, -bound, bound).astype(held_as)


def setup_inputs(seed: int = 0) -> dict:
    key_list = jax.random.split(jax.random.key(seed), 8)
    tokens = draw_tokens(jax.random.fold_in(key_list[7], 71), 0)
    slot_keys = draw_slot_keys(jax.random.fold_in(key_list[7], 71), 0)
    logit_scale = jnp.clip(jnp.exp(jax.random.uniform(key_list[2], (1,), jnp.float32, math.log(8.0), math.log(16.0))), 8.0, 16.0)
    up_weight = bell_draw(key_list[3], (EXPERTS, D, FF), D ** -0.5, 0.15625, ((0, 8), (2, 4)))
    up_bias = bell_draw(key_list[4], (EXPERTS, FF), 0.5, 3.0, ((0, 8), (1, 4)))
    down_weight = bell_draw(key_list[5], (EXPERTS, FF, D), FF ** -0.5, 0.078125, ((0, 8), (1, 4)))
    down_bias = bell_draw(key_list[6], (EXPERTS, D), 0.5, 3.0)
    return dict(tokens=tokens, slot_keys=slot_keys, logit_scale=logit_scale, up_weight=up_weight, up_bias=up_bias, down_weight=down_weight, down_bias=down_bias)


norm_eps = 1e-06

def unit_rms(values, axis_pos):
    return values * lax.rsqrt(lax.optimization_barrier(jnp.mean(values * values, axis=axis_pos, keepdims=True)) + norm_eps)

def reference(tokens, slot_keys, logit_scale, up_weight, up_bias, down_weight, down_bias):
    normed_tok = unit_rms(tokens.astype(jnp.float32), 2).astype(jnp.bfloat16)
    normed_keys = unit_rms(slot_keys.astype(jnp.float32), 0).astype(jnp.bfloat16)
    raw_scores = jnp.einsum('ipd,dn->inp', normed_tok.astype(jnp.float32), normed_keys.astype(jnp.float32))
    logits = logit_scale[0] * raw_scores / D
    dispatch = jax.nn.softmax(logits, axis=2).astype(jnp.bfloat16)
    combine = jax.nn.softmax(logits, axis=1).astype(jnp.bfloat16)
    slot_inputs = jnp.einsum('inp,ipd->ind', dispatch.astype(jnp.float32), tokens.astype(jnp.float32)).astype(jnp.bfloat16)

    def one_expert(packed):
        slot_rows, weight_in, bias_in, weight_out = packed
        pre = jnp.dot(slot_rows, weight_in, preferred_element_type=jnp.float32) + bias_in.astype(jnp.float32)[None, :]
        hidden = jax.nn.gelu(pre, approximate=False).astype(jnp.bfloat16)
        blocks = FF // N_DP
        hidden_blocks = jnp.transpose(hidden.reshape(IMAGES, N_DP, blocks), (1, 0, 2))
        weight_blocks = weight_out.reshape(N_DP, blocks, D)
        parts = jnp.einsum('gif,gfd->gid', hidden_blocks.astype(jnp.float32), weight_blocks.astype(jnp.float32))
        parts = parts.astype(jnp.bfloat16)
        return lax.optimization_barrier(jnp.sum(parts.astype(jnp.float32), axis=0))
    summed = lax.map(one_expert, (jnp.transpose(slot_inputs, (1, 0, 2)), up_weight, up_bias, down_weight))
    expert_out = (summed + down_bias.astype(jnp.float32)[:, None, :]).astype(jnp.bfloat16)
    mixed_out = jnp.einsum('inp,nid->ipd', combine.astype(jnp.float32), expert_out.astype(jnp.float32))
    return mixed_out.astype(jnp.bfloat16)
```

```python
import functools

import jax
import jax.numpy as jnp
from jax import lax
from jax.experimental import pallas as pl
from jax.experimental.pallas import tpu as pltpu
from jax.sharding import PartitionSpec as P

MESH = pl.DeviceIdType.MESH
F32 = jnp.float32
BF16 = jnp.bfloat16
norm_eps = 1e-06
NT = (((1,), (1,)), ((), ()))
CORES = 2
BANDS = 4
LOG2E = 1.4426950408889634


def erf_gelu(v):
    return 0.5 * v * (1.0 + lax.erf(v * 0.7071067811865476))


def row_squares(t):
    patches, width = t.shape
    s = jnp.zeros((patches, 128), F32)
    for j in range(0, width, 128):
        u = t[:, j : j + 128].astype(F32)
        s = s + u * u
    hi = s.astype(BF16)
    lo = (s - hi.astype(F32)).astype(BF16)
    both = jnp.concatenate([hi, lo], axis=1)
    ones = jnp.ones((16, 256), BF16)
    return lax.dot_general(ones, both, NT, preferred_element_type=F32)[0:1]


def route_and_experts(
    owners,
    n_dp,
    chunk,
    cuts,
    tok_hbm,
    keys_hbm,
    scale_hbm,
    w1_hbm,
    b1_hbm,
    w2_hbm,
    b2_hbm,
    comb_ref,
    ret_ref,
    keys_ref,
    scale_ref,
    b1_ref,
    b2_ref,
    tok,
    w1,
    w2,
    send,
    recv,
    xf,
    hid,
    part,
    mine,
    pair,
    back,
    got,
    load_sem,
    tok_sem,
    sent_sem,
    band_sem,
    land_sem,
    p_recv,
):
    images, patches, width = tok.shape
    hidden = w1.shape[1]
    halves = n_dp // CORES
    groups = halves * owners
    per = groups // BANDS
    rows = groups * images
    slots = owners * images

    d = lax.axis_index("dp")
    e = lax.axis_index("expert")
    core = lax.rem(d, CORES)
    half = lax.div(d, CORES)
    me = e * halves + half
    band = lax.div(e, owners // BANDS)
    other = 1 - core
    partner = {"dp": half * CORES + other, "expert": e}

    low = band < BANDS // 2
    near = [
        band,
        band + 1 - 2 * lax.rem(band, 2),
        jnp.where(low, 2, 1),
        jnp.where(low, 3, 0),
    ]

    def for_band(act, b):
        if per <= 8:
            for m in range(per):
                ee = b * (per // halves) + m // halves
                dev = {"dp": (m % halves) * CORES + other, "expert": ee}
                act(b * per + m, dev)
        else:

            def step(m, c):
                t = b * per + m
                dev = {
                    "dp": lax.rem(t, halves) * CORES + other,
                    "expert": lax.div(t, halves),
                }
                act(t, dev)
                return c

            lax.fori_loop(0, per, step, 0)

    load_keys = pltpu.make_async_copy(keys_hbm, keys_ref, load_sem.at[0])
    load_scale = pltpu.make_async_copy(scale_hbm, scale_ref, load_sem.at[1])
    load_b1 = pltpu.make_async_copy(b1_hbm, b1_ref, load_sem.at[2])
    load_b2 = pltpu.make_async_copy(b2_hbm, b2_ref, load_sem.at[2])
    load1 = pltpu.make_async_copy(w1_hbm.at[0], w1, load_sem.at[2])
    load2 = pltpu.make_async_copy(w2_hbm.at[0], w2, load_sem.at[3])

    def load_tok(i):
        return pltpu.make_async_copy(tok_hbm.at[i], tok.at[i], tok_sem.at[i])

    load_keys.start()
    load_scale.start()
    for i in range(images):
        load_tok(i).start()
    barrier = pltpu.get_barrier_semaphore()

    def greet(t, dev):
        pl.semaphore_signal(barrier, inc=1, device_id=dev, device_id_type=MESH)

    for b in near[::-1]:
        for_band(greet, b)

    load_keys.wait()
    slot_of = lax.broadcasted_iota(jnp.int32, (slots, owners), 0) // images
    col = lax.broadcasted_iota(jnp.int32, (slots, owners), 1)
    spread = jnp.where(slot_of == col, 1.0, 0.0).astype(BF16)
    keys = jnp.dot(spread, keys_ref[...], preferred_element_type=F32)
    load_scale.wait()
    key_scale = lax.rsqrt(jnp.mean(keys * keys, axis=1, keepdims=True) + norm_eps)
    key_scale = key_scale * (scale_ref[0] * (LOG2E / width))
    keys = keys.astype(BF16)
    image_of = lax.broadcasted_iota(jnp.int32, (slots, patches), 0) % images

    total = jnp.zeros((slots, width), F32)
    summed = jnp.zeros((slots, patches), F32)
    raw, inv, powers = [], [], []

    def dispatch(i, total, summed):
        power = jnp.exp2(raw[i] * key_scale * inv[i])
        powers.append(power)
        picked = jnp.where(image_of == i, power, 0.0)
        total = total + jnp.dot(
            picked.astype(BF16), tok[i], preferred_element_type=F32
        )
        return total, summed + picked

    for i in range(images):
        load_tok(i).wait()
        t = tok[i]
        raw.append(lax.dot_general(keys, t, NT, preferred_element_type=F32))
        inv.append(lax.rsqrt(row_squares(t) / width + norm_eps))
        if i == images - 1:
            load1.start()
            load2.start()
            load_b1.start()
            load_b2.start()
        if i > 0:
            total, summed = dispatch(i - 1, total, summed)
    total, summed = dispatch(images - 1, total, summed)
    total = total * (1.0 / jnp.sum(summed, axis=1, keepdims=True))
    for n in range(owners):
        send[n] = total[n * images : (n + 1) * images].astype(BF16)

    pl.semaphore_wait(barrier, groups)

    def start_out(t, dev):
        pltpu.make_async_remote_copy(
            src_ref=send.at[lax.div(t, halves)],
            dst_ref=recv.at[core, me],
            send_sem=sent_sem.at[0],
            recv_sem=band_sem.at[band],
            device_id=dev,
            device_id_type=MESH,
        ).start()

    for b in near[::-1]:
        for_band(start_out, b)

    for i in range(images):
        mix = powers[i] * (images / jnp.sum(powers[i], axis=0, keepdims=True))
        comb_ref[i] = jnp.where(image_of == i, mix, 0.0).T.astype(BF16)

    def relay(b):
        block = recv.at[other, pl.ds(b * per, per)]
        return pltpu.make_async_remote_copy(
            src_ref=block,
            dst_ref=block,
            send_sem=sent_sem.at[1],
            recv_sem=land_sem.at[0],
            device_id=partner,
            device_id_type=MESH,
        )

    def whole(ref, send_sem, recv_sem):
        return pltpu.make_async_remote_copy(
            src_ref=ref,
            dst_ref=ref,
            send_sem=send_sem,
            recv_sem=recv_sem,
            device_id=partner,
            device_id_type=MESH,
        )

    for b in near:
        block = recv.at[other, pl.ds(b * per, per)]
        whole(block, sent_sem.at[0], band_sem.at[b]).wait_recv()
        relay(b).start()

    whole(recv.at[0], sent_sem.at[0], land_sem.at[0]).wait_recv()

    for side in range(CORES):

        def place(k, c):
            pairs = [recv[side, 2 * k + q].astype(F32) for q in range(2)]
            at = pl.multiple_of(side * rows + k * 2 * images, 2 * images)
            xf[pl.ds(at, 2 * images), :] = jnp.concatenate(pairs, axis=0)
            return c

        lax.fori_loop(0, groups // 2, place, 0, unroll=groups <= 16)

    load1.wait()
    load_b1.wait()
    load_b2.wait()
    block = min(128, CORES * rows)
    steps = CORES * rows // block

    def first(m, c):
        at = pl.multiple_of(m * block, block)
        x = xf[pl.ds(at, block), :].astype(BF16)
        for j in range(0, hidden, chunk):
            v = jnp.dot(x, w1[:, j : j + chunk], preferred_element_type=F32)
            v = v + b1_ref[0:1, j : j + chunk].astype(F32)
            hid[pl.ds(at, block), j : j + chunk] = erf_gelu(v).astype(BF16)
        return c

    lax.fori_loop(0, steps, first, 0, unroll=steps == 1)
    load2.wait()

    def pair_copy(k):
        lo, hi = cuts[k], cuts[k + 1]
        at = pl.multiple_of(core * rows, rows)
        return pltpu.make_async_remote_copy(
            src_ref=part.at[pl.ds(at, rows), lo:hi],
            dst_ref=pair.at[:, lo:hi],
            send_sem=sent_sem.at[2],
            recv_sem=p_recv.at[k],
            device_id=partner,
            device_id_type=MESH,
        )

    for k in range(len(cuts) - 1):

        def second(m, c):
            at = pl.multiple_of(m * block, block)
            h = hid[pl.ds(at, block), :]
            for j in range(cuts[k], cuts[k + 1], chunk):
                v = jnp.dot(h, w2[:, j : j + chunk], preferred_element_type=F32)
                part[pl.ds(at, block), j : j + chunk] = v.astype(BF16)
                mine[pl.ds(at, block), j : j + chunk] = v
            return c

        lax.fori_loop(0, steps, second, 0, unroll=steps == 1)
        pair_copy(k).start()

    for k in range(len(cuts) - 1):
        lo, hi = cuts[k], cuts[k + 1]
        pair_copy(k).wait_recv()

        def join(q, c):
            at = pl.multiple_of(q * 4 * images, 4 * images)
            own_at = pl.multiple_of(other * rows + at, 4 * images)
            v = mine[pl.ds(own_at, 4 * images), lo:hi]
            v = v + pair[pl.ds(at, 4 * images), lo:hi].astype(F32)
            for r in range(4):
                back[4 * q + r, :, lo:hi] = v[r * images : (r + 1) * images].astype(
                    BF16
                )
            return c

        lax.fori_loop(0, groups // 4, join, 0, unroll=groups <= 16)

    def start_home(t, dev):
        pltpu.make_async_remote_copy(
            src_ref=back.at[t],
            dst_ref=got.at[me],
            send_sem=sent_sem.at[3],
            recv_sem=land_sem.at[1],
            device_id=dev,
            device_id_type=MESH,
        ).start()

    for b in near[::-1]:
        for_band(start_home, b)

    whole(recv.at[0], sent_sem.at[0], land_sem.at[0]).wait_send()
    whole(recv.at[0], sent_sem.at[1], land_sem.at[0]).wait_send()
    for k in range(len(cuts) - 1):
        pair_copy(k).wait_send()
    whole(back, sent_sem.at[3], land_sem.at[1]).wait_send()
    whole(got, sent_sem.at[3], land_sem.at[1]).wait_recv()
    bias = b2_ref[...].astype(F32)
    for n in range(0, owners, 4):
        four = []
        for q in range(n, n + 4):
            v = got[q * halves].astype(F32)
            for x in range(1, halves):
                v = v + got[q * halves + x].astype(F32)
            four.append(v + bias[q : q + 1])
        block = jnp.concatenate(four, axis=0)
        ret_ref[n * images : (n + 4) * images, :] = block.astype(BF16)


def mix_kernel(pieces, comb_ref, ret_ref, out_ref, out, out_sem):
    images, patches, _ = comb_ref.shape
    step = patches // pieces
    ret = ret_ref[...]
    copies = []
    for i in range(images):
        for k in range(pieces):
            at = pl.ds(k * step, step)
            v = jnp.dot(comb_ref[i, at], ret, preferred_element_type=F32)
            out[i, at] = v.astype(out.dtype)
            copies.append(
                pltpu.make_async_copy(out.at[i, at], out_ref.at[i, at], out_sem.at[0])
            )
            copies[-1].start()
    for copy in copies:
        copy.wait()


def body(tokens, slot_keys, logit_scale, up_weight, up_bias, down_weight, down_bias):
    images, patches, width = tokens.shape
    owners = lax.axis_size("expert")
    n_dp = lax.axis_size("dp")
    hidden = up_weight.shape[2]
    halves = n_dp // CORES
    groups = halves * owners
    rows = groups * images
    slots = owners * images
    chunk = 256
    middle = (width // chunk + 1) // 2 * chunk
    cuts = (0, middle, width)
    vmem = pl.BlockSpec(memory_space=pltpu.VMEM)
    hbm = pl.BlockSpec(memory_space=pl.ANY)
    dma = pltpu.SemaphoreType.DMA
    comb, ret = pl.pallas_call(
        functools.partial(route_and_experts, owners, n_dp, chunk, cuts),
        out_shape=(
            pltpu.VMEM((images, patches, slots), BF16),
            pltpu.VMEM((slots, width), BF16),
        ),
        in_specs=[
            hbm,
            hbm,
            pl.BlockSpec(memory_space=pltpu.HBM),
            hbm,
            hbm,
            hbm,
            hbm,
        ],
        out_specs=(vmem, vmem),
        scratch_shapes=[
            pltpu.VMEM((owners, width), BF16),
            pltpu.SMEM((1,), F32),
            pltpu.VMEM(up_bias.shape, BF16),
            pltpu.VMEM(down_bias.shape, BF16),
            pltpu.VMEM((images, patches, width), BF16),
            pltpu.VMEM((width, hidden), BF16),
            pltpu.VMEM((hidden, width), BF16),
            pltpu.VMEM((owners, images, width), BF16),
            pltpu.VMEM((CORES, groups, images, width), BF16),
            pltpu.VMEM((CORES * rows, width), F32),
            pltpu.VMEM((CORES * rows, hidden), BF16),
            pltpu.VMEM((CORES * rows, width), BF16),
            pltpu.VMEM((CORES * rows, width), F32),
            pltpu.VMEM((rows, width), BF16),
            pltpu.VMEM((groups, images, width), BF16),
            pltpu.VMEM((groups, images, width), BF16),
            dma((4,)),
            dma((images,)),
            dma((4,)),
            dma((BANDS,)),
            dma((2,)),
            dma((len(cuts) - 1,)),
        ],
        compiler_params=pltpu.CompilerParams(
            collective_id=0, has_side_effects=True, vmem_limit_bytes=60 * 1024 * 1024
        ),
        name="route_and_experts",
    )(tokens, slot_keys.T, logit_scale, up_weight, up_bias, down_weight, down_bias)
    return pl.pallas_call(
        functools.partial(mix_kernel, 2),
        out_shape=jax.ShapeDtypeStruct(tokens.shape, BF16),
        in_specs=[vmem, vmem],
        out_specs=hbm,
        scratch_shapes=[pltpu.VMEM(tokens.shape, BF16), dma((1,))],
        name="mix_tokens",
    )(
        pltpu.with_memory_space_constraint(comb, pltpu.VMEM),
        pltpu.with_memory_space_constraint(ret, pltpu.VMEM),
    )


def solution(mesh):
    return jax.shard_map(
        body,
        mesh=mesh,
        in_specs=(
            P(("dp", "expert"), None, None),
            P(),
            P(),
            P("expert", None, "dp"),
            P("expert", "dp"),
            P("expert", "dp", None),
            P(),
        ),
        out_specs=P(("dp", "expert"), None, None),
        check_vma=False,
    )
```

```python
import functools

import jax
import jax.numpy as jnp
from jax import lax
from jax.experimental import pallas as pl
from jax.experimental.pallas import tpu as pltpu
from jax.sharding import PartitionSpec as P

MESH = pl.DeviceIdType.MESH
F32 = jnp.float32
BF16 = jnp.bfloat16
norm_eps = 1e-06
NT = (((1,), (1,)), ((), ()))
CORES = 2
BANDS = 4
LOG2E = 1.4426950408889634


def erf_gelu(v):
    return 0.5 * v * (1.0 + lax.erf(v * 0.7071067811865476))


def row_squares(t):
    patches, width = t.shape
    s = jnp.zeros((patches, 128), F32)
    for j in range(0, width, 128):
        u = t[:, j : j + 128].astype(F32)
        s = s + u * u
    return jnp.sum(s.T, axis=0, keepdims=True)


def scores(keys, t):
    middle = t.shape[0] // 2
    return jnp.concatenate(
        [
            lax.dot_general(keys, u, NT, preferred_element_type=F32)
            for u in (t[:middle], t[middle:])
        ],
        axis=1,
    )


def route_and_experts(
    owners,
    n_dp,
    chunk,
    cuts,
    tok_hbm,
    keys_hbm,
    scale_hbm,
    w1_hbm,
    b1_hbm,
    w2_hbm,
    b2_hbm,
    comb_ref,
    ret_ref,
    keys_ref,
    scale_ref,
    b1_ref,
    b2_ref,
    tok,
    w1,
    w2,
    send,
    recv,
    xf,
    hid,
    part,
    mine,
    pair,
    back,
    got,
    load_sem,
    tok_sem,
    sent_sem,
    band_sem,
    land_sem,
    p_recv,
):
    images, patches, width = tok.shape
    hidden = w1.shape[1]
    halves = n_dp // CORES
    groups = halves * owners
    per = groups // BANDS
    rows = groups * images
    slots = owners * images

    d = lax.axis_index("dp")
    e = lax.axis_index("expert")
    core = lax.rem(d, CORES)
    half = lax.div(d, CORES)
    me = e * halves + half
    band = lax.div(e, owners // BANDS)
    other = 1 - core
    partner = {"dp": half * CORES + other, "expert": e}

    low = band < BANDS // 2
    near = [
        band,
        band + 1 - 2 * lax.rem(band, 2),
        jnp.where(low, 2, 1),
        jnp.where(low, 3, 0),
    ]

    def for_band(act, b):
        if per <= 8:
            for m in range(per):
                ee = b * (per // halves) + m // halves
                dev = {"dp": (m % halves) * CORES + other, "expert": ee}
                act(b * per + m, dev)
        else:

            def step(m, c):
                t = b * per + m
                dev = {
                    "dp": lax.rem(t, halves) * CORES + other,
                    "expert": lax.div(t, halves),
                }
                act(t, dev)
                return c

            lax.fori_loop(0, per, step, 0)

    load_keys = pltpu.make_async_copy(keys_hbm, keys_ref, load_sem.at[0])
    load_scale = pltpu.make_async_copy(scale_hbm, scale_ref, load_sem.at[1])
    load_b1 = pltpu.make_async_copy(b1_hbm, b1_ref, load_sem.at[2])
    load_b2 = pltpu.make_async_copy(b2_hbm, b2_ref, load_sem.at[2])
    load1 = pltpu.make_async_copy(w1_hbm.at[0], w1, load_sem.at[2])
    load2 = pltpu.make_async_copy(w2_hbm.at[0], w2, load_sem.at[3])

    def load_tok(i):
        return pltpu.make_async_copy(tok_hbm.at[i], tok.at[i], tok_sem.at[i])

    load_keys.start()
    load_scale.start()
    for i in range(images):
        load_tok(i).start()
    barrier = pltpu.get_barrier_semaphore()

    def greet(t, dev):
        pl.semaphore_signal(barrier, inc=1, device_id=dev, device_id_type=MESH)

    for b in near[::-1]:
        for_band(greet, b)

    image_of = lax.broadcasted_iota(jnp.int32, (slots, patches), 0) % images
    total = jnp.zeros((slots, width), F32)
    summed = jnp.zeros((slots, patches), F32)
    raw, inv, shares = [], [], []

    def dispatch(i, total, summed):
        power = jnp.exp2(raw[i] * key_scale * inv[i])
        share = 1.0 / jnp.sum(power, axis=0, keepdims=True)
        power = jnp.concatenate(
            [
                jnp.broadcast_to(power[n : n + 1], (images, patches))
                for n in range(owners)
            ],
            axis=0,
        )
        picked = jnp.where(image_of == i, power, 0.0)
        shares.append(picked * share)
        total = total + jnp.dot(
            picked.astype(BF16), tok[i], preferred_element_type=F32
        )
        return total, summed + picked

    load_keys.wait()
    load_scale.wait()
    keys = keys_ref[...]
    wide = keys.astype(F32)
    key_scale = lax.rsqrt(jnp.mean(wide * wide, axis=1, keepdims=True) + norm_eps)
    key_scale = key_scale * (scale_ref[0] * (LOG2E / width))
    for i in range(images):
        load_tok(i).wait()
        t = tok[i]
        raw.append(scores(keys, t))
        inv.append(lax.rsqrt(row_squares(t) / width + norm_eps))
        if i == images - 1:
            load1.start()
            load2.start()
            load_b1.start()
            load_b2.start()
        if i > 0:
            total, summed = dispatch(i - 1, total, summed)
    total, summed = dispatch(images - 1, total, summed)
    total = total * (1.0 / jnp.sum(summed, axis=1, keepdims=True))
    for n in range(owners):
        send[n] = total[n * images : (n + 1) * images].astype(BF16)

    pl.semaphore_wait(barrier, groups)

    def start_out(t, dev):
        pltpu.make_async_remote_copy(
            src_ref=send.at[lax.div(t, halves)],
            dst_ref=recv.at[core, me],
            send_sem=sent_sem.at[0],
            recv_sem=band_sem.at[band],
            device_id=dev,
            device_id_type=MESH,
        ).start()

    for b in near[::-1]:
        for_band(start_out, b)

    for i in range(images):
        comb_ref[i] = shares[i].T.astype(BF16)

    def relay(b):
        block = recv.at[other, pl.ds(b * per, per)]
        return pltpu.make_async_remote_copy(
            src_ref=block,
            dst_ref=block,
            send_sem=sent_sem.at[1],
            recv_sem=land_sem.at[0],
            device_id=partner,
            device_id_type=MESH,
        )

    def whole(ref, send_sem, recv_sem):
        return pltpu.make_async_remote_copy(
            src_ref=ref,
            dst_ref=ref,
            send_sem=send_sem,
            recv_sem=recv_sem,
            device_id=partner,
            device_id_type=MESH,
        )

    for b in near:
        block = recv.at[other, pl.ds(b * per, per)]
        whole(block, sent_sem.at[0], band_sem.at[b]).wait_recv()
        relay(b).start()

    whole(recv.at[0], sent_sem.at[0], land_sem.at[0]).wait_recv()

    for side in range(CORES):

        def place(k, c):
            pairs = [recv[side, 2 * k + q].astype(F32) for q in range(2)]
            at = pl.multiple_of(side * rows + k * 2 * images, 2 * images)
            xf[pl.ds(at, 2 * images), :] = jnp.concatenate(pairs, axis=0)
            return c

        lax.fori_loop(0, groups // 2, place, 0, unroll=groups <= 16)

    load1.wait()
    load_b1.wait()
    load_b2.wait()
    block = min(128, CORES * rows)
    steps = CORES * rows // block

    def first(m, c):
        at = pl.multiple_of(m * block, block)
        x = xf[pl.ds(at, block), :].astype(BF16)
        for j in range(0, hidden, chunk):
            v = jnp.dot(x, w1[:, j : j + chunk], preferred_element_type=F32)
            v = v + b1_ref[0:1, j : j + chunk].astype(F32)
            hid[pl.ds(at, block), j : j + chunk] = erf_gelu(v).astype(BF16)
        return c

    lax.fori_loop(0, steps, first, 0, unroll=steps == 1)
    load2.wait()

    def pair_copy(k):
        lo, hi = cuts[k], cuts[k + 1]
        at = pl.multiple_of(core * rows, rows)
        return pltpu.make_async_remote_copy(
            src_ref=part.at[pl.ds(at, rows), lo:hi],
            dst_ref=pair.at[:, lo:hi],
            send_sem=sent_sem.at[2],
            recv_sem=p_recv.at[k],
            device_id=partner,
            device_id_type=MESH,
        )

    for k in range(len(cuts) - 1):

        def second(m, c):
            at = pl.multiple_of(m * block, block)
            h = hid[pl.ds(at, block), :]
            for j in range(cuts[k], cuts[k + 1], chunk):
                v = jnp.dot(h, w2[:, j : j + chunk], preferred_element_type=F32)
                part[pl.ds(at, block), j : j + chunk] = v.astype(BF16)
                mine[pl.ds(at, block), j : j + chunk] = v
            return c

        lax.fori_loop(0, steps, second, 0, unroll=steps == 1)
        pair_copy(k).start()

    for k in range(len(cuts) - 1):
        lo, hi = cuts[k], cuts[k + 1]
        pair_copy(k).wait_recv()

        def join(q, c):
            at = pl.multiple_of(q * 4 * images, 4 * images)
            own_at = pl.multiple_of(other * rows + at, 4 * images)
            v = mine[pl.ds(own_at, 4 * images), lo:hi]
            v = v + pair[pl.ds(at, 4 * images), lo:hi].astype(F32)
            for r in range(4):
                back[4 * q + r, :, lo:hi] = v[r * images : (r + 1) * images].astype(
                    BF16
                )
            return c

        lax.fori_loop(0, groups // 4, join, 0, unroll=groups <= 16)

    def start_home(t, dev):
        pltpu.make_async_remote_copy(
            src_ref=back.at[t],
            dst_ref=got.at[me],
            send_sem=sent_sem.at[3],
            recv_sem=land_sem.at[1],
            device_id=dev,
            device_id_type=MESH,
        ).start()

    for b in near[::-1]:
        for_band(start_home, b)

    whole(recv.at[0], sent_sem.at[0], land_sem.at[0]).wait_send()
    whole(recv.at[0], sent_sem.at[1], land_sem.at[0]).wait_send()
    for k in range(len(cuts) - 1):
        pair_copy(k).wait_send()
    whole(back, sent_sem.at[3], land_sem.at[1]).wait_send()
    whole(got, sent_sem.at[3], land_sem.at[1]).wait_recv()
    bias = b2_ref[...].astype(F32)
    for n in range(0, owners, 4):
        four = []
        for q in range(n, n + 4):
            v = got[q * halves].astype(F32)
            for x in range(1, halves):
                v = v + got[q * halves + x].astype(F32)
            four.append(v + bias[q : q + 1])
        block = jnp.concatenate(four, axis=0)
        ret_ref[n * images : (n + 4) * images, :] = block.astype(BF16)


def mix_kernel(pieces, comb_ref, ret_ref, out_ref, out, out_sem):
    images, patches, _ = comb_ref.shape
    step = patches // pieces
    ret = ret_ref[...]
    copies = []
    for i in range(images):
        for k in range(pieces):
            at = pl.ds(k * step, step)
            v = jnp.dot(comb_ref[i, at], ret, preferred_element_type=F32)
            out[i, at] = v.astype(out.dtype)
            copies.append(
                pltpu.make_async_copy(out.at[i, at], out_ref.at[i, at], out_sem.at[0])
            )
            copies[-1].start()
    for copy in copies:
        copy.wait()


def body(tokens, slot_keys, logit_scale, up_weight, up_bias, down_weight, down_bias):
    images, patches, width = tokens.shape
    owners = lax.axis_size("expert")
    n_dp = lax.axis_size("dp")
    hidden = up_weight.shape[2]
    halves = n_dp // CORES
    groups = halves * owners
    rows = groups * images
    slots = owners * images
    chunk = 256
    middle = (width // chunk + 1) // 2 * chunk
    cuts = (0, middle, width)
    vmem = pl.BlockSpec(memory_space=pltpu.VMEM)
    hbm = pl.BlockSpec(memory_space=pl.ANY)
    dma = pltpu.SemaphoreType.DMA
    comb, ret = pl.pallas_call(
        functools.partial(route_and_experts, owners, n_dp, chunk, cuts),
        out_shape=(
            pltpu.VMEM((images, patches, slots), BF16),
            pltpu.VMEM((slots, width), BF16),
        ),
        in_specs=[
            hbm,
            hbm,
            pl.BlockSpec(memory_space=pltpu.HBM),
            hbm,
            hbm,
            hbm,
            hbm,
        ],
        out_specs=(vmem, vmem),
        scratch_shapes=[
            pltpu.VMEM((owners, width), BF16),
            pltpu.SMEM((1,), F32),
            pltpu.VMEM(up_bias.shape, BF16),
            pltpu.VMEM(down_bias.shape, BF16),
            pltpu.VMEM((images, patches, width), BF16),
            pltpu.VMEM((width, hidden), BF16),
            pltpu.VMEM((hidden, width), BF16),
            pltpu.VMEM((owners, images, width), BF16),
            pltpu.VMEM((CORES, groups, images, width), BF16),
            pltpu.VMEM((CORES * rows, width), F32),
            pltpu.VMEM((CORES * rows, hidden), BF16),
            pltpu.VMEM((CORES * rows, width), BF16),
            pltpu.VMEM((CORES * rows, width), F32),
            pltpu.VMEM((rows, width), BF16),
            pltpu.VMEM((groups, images, width), BF16),
            pltpu.VMEM((groups, images, width), BF16),
            dma((4,)),
            dma((images,)),
            dma((4,)),
            dma((BANDS,)),
            dma((2,)),
            dma((len(cuts) - 1,)),
        ],
        compiler_params=pltpu.CompilerParams(
            collective_id=0, has_side_effects=True, vmem_limit_bytes=60 * 1024 * 1024
        ),
        name="route_and_experts",
    )(tokens, slot_keys.T, logit_scale, up_weight, up_bias, down_weight, down_bias)
    return pl.pallas_call(
        functools.partial(mix_kernel, 2),
        out_shape=jax.ShapeDtypeStruct(tokens.shape, BF16),
        in_specs=[vmem, vmem],
        out_specs=hbm,
        scratch_shapes=[pltpu.VMEM(tokens.shape, BF16), dma((1,))],
        name="mix_tokens",
    )(
        pltpu.with_memory_space_constraint(comb, pltpu.VMEM),
        pltpu.with_memory_space_constraint(ret, pltpu.VMEM),
    )


def solution(mesh):
    return jax.shard_map(
        body,
        mesh=mesh,
        in_specs=(
            P(("dp", "expert"), None, None),
            P(),
            P(),
            P("expert", None, "dp"),
            P("expert", "dp"),
            P("expert", "dp", None),
            P(),
        ),
        out_specs=P(("dp", "expert"), None, None),
        check_vma=False,
    )
```
